32 devices in a mesh: dp: 2 (over z, core), tp: 16 (over x, y).
Axes of the slice: x: 4, y: 4, z: 1, core: 2. Of those that a mesh axis runs over, the one named last changes fastest.
The devices are a block of a 4x4x8 slice.
Arguments:
- x: bfloat16 [4096, 8192], P(('dp', 'tp')), parts along dimension 0
- dy: bfloat16 [4096, 8192], P(('dp', 'tp')), parts along dimension 0
- gate: bfloat16 [4096, 24576], P('dp', 'tp'), parts along dimension 0
- up: bfloat16 [4096, 24576], P('dp', 'tp'), parts along dimension 0
- w_gate: bfloat16 [8192, 24576], P(None, 'tp')
- w_up: bfloat16 [8192, 24576], P(None, 'tp')
- w_down: bfloat16 [24576, 8192], P('tp')
Outputs:
- output 1: bfloat16 [4096, 8192], P(('dp', 'tp')), parts along dimension 0
- output 2: bfloat16 [16384, 24576], P('dp', 'tp'), parts along dimension 0
- output 3: bfloat16 [16384, 24576], P('dp', 'tp'), parts along dimension 0
- output 4: bfloat16 [49152, 8192], P(('dp', 'tp')), parts along dimension 0
There are 2 independent parts. The reference program is written for one: setup_inputs(seed, part) draws one part's arguments, and reference() takes and returns one part's arrays. A program takes and returns all parts, laid end to end along the dimension named above; an argument that names none is the same for every part.
All inputs are finite; a program needn't handle non-finite values.
Results may differ from the reference program's by a relative error of at most 0.012.
Values are sent between devices in bfloat16 or wider.
A program may use at most 768 MiB of HBM per device.

```python
import jax
import jax.numpy as jnp

ROWS = 2048
D = 8192
FF = 24576


def act(gate, up):
    return jax.nn.silu(gate) * up


def setup_inputs(seed: int = 0, part: int = 0) -> dict:
    kx, ky, ka, kb, kg, ku, kd = jax.random.split(jax.random.key(seed), 7)
    kx, ky, ka, kb = (jax.random.fold_in(k, part) for k in (kx, ky, ka, kb))
    drawn = {
        "x": jax.random.normal(kx, (ROWS, D), jnp.float32),
        "dy": jax.random.normal(ky, (ROWS, D), jnp.float32),
        "gate": jax.random.normal(ka, (ROWS, FF), jnp.float32),
        "up": jax.random.normal(kb, (ROWS, FF), jnp.float32),
        "w_gate": jax.random.normal(kg, (D, FF), jnp.float32) * D**-0.5,
        "w_up": jax.random.normal(ku, (D, FF), jnp.float32) * D**-0.5,
        "w_down": jax.random.normal(kd, (FF, D), jnp.float32) * FF**-0.5,
    }
    return {k: v.astype(jnp.bfloat16) for k, v in drawn.items()}


def reference(x, dy, gate, up, w_gate, w_up, w_down):
    hidden, back = jax.vjp(act, gate.astype(jnp.float32), up.astype(jnp.float32))
    d_hidden = jnp.dot(dy, w_down.T, preferred_element_type=jnp.float32)
    d_gate, d_up = (g.astype(jnp.bfloat16) for g in back(d_hidden))
    dx = jnp.dot(d_gate, w_gate.T, preferred_element_type=jnp.float32) + jnp.dot(d_up, w_up.T, preferred_element_type=jnp.float32)
    dw_gate = jnp.dot(x.T, d_gate, preferred_element_type=jnp.float32)
    dw_up = jnp.dot(x.T, d_up, preferred_element_type=jnp.float32)
    dw_down = jnp.dot(hidden.astype(jnp.bfloat16).T, dy, preferred_element_type=jnp.float32)
    return tuple(g.astype(jnp.bfloat16) for g in (dx, dw_gate, dw_up, dw_down))
```

```python
import functools
import math

import jax
import jax.numpy as jnp
from jax import lax
from jax.experimental import pallas as pl
from jax.experimental.pallas import tpu as pltpu
from jax.sharding import PartitionSpec as P

RINGS = 4
SUBS = 4
BF16 = jnp.bfloat16
F32 = jnp.float32
NT = (((1,), (1,)), ((), ()))
TN = (((0,), (0,)), ((), ()))


def act_grads(g, u, dh):
    sig = jax.nn.sigmoid(g)
    silu = g * sig
    ds = dh * u
    return silu * u, ds * (sig + silu * (1.0 - sig)), dh * silu


def gather_kernel(
    n, tile_f, tile_d,
    x_ref, dy_ref, gate_ref, up_ref, wg_ref, wu_ref, wd_ref,
    full_ref, dg_ref, du_ref, hid_ref, dx_ref,
    blk, wd_buf, w2_buf, gu_buf, dh_buf, grads, obuf,
    send_sem, recv_sem, blk_sem, wd_sem, w2_sem, gu_sem, grads_sem, o_sem,
):
    side = math.isqrt(n)
    rows, d_model = x_ref.shape
    ff = gate_ref.shape[1]
    piece = rows // RINGS
    sub_rows = piece // SUBS
    hops = n - 1
    per_block = blk.shape[0] // rows
    blocks = n // per_block
    tiles_a = ff // tile_f
    tiles_b = d_model // tile_d
    tiles = tiles_a + tiles_b
    messages = 2 * hops * SUBS

    me = lax.axis_index("tp")
    a, b = me // side, me % side
    place = (a * side + (a + b) % side, b * side + (a + b) % side)

    def device(ring, k):
        k = (k + 2 * n) % n
        u = k // side
        v = (k - u) % side
        return u * side + v if ring // 2 == 0 else v * side + u

    def owner(ring, distance):
        return device(ring, place[ring // 2] - distance if ring % 2 == 0 else place[ring // 2] + distance)

    def following(ring):
        return owner(ring, -1)

    def rows_of(ring, distance):
        return pl.multiple_of(owner(ring, distance) * rows + ring * piece, piece)

    barrier = pltpu.get_barrier_semaphore()
    for ring in range(RINGS):
        pl.semaphore_signal(barrier, inc=1, device_id={"tp": following(ring)}, device_id_type=pl.DeviceIdType.MESH)
    pl.semaphore_wait(barrier, RINGS)

    def message(ring, src, which, distance, sub, index):
        start = pl.multiple_of(rows_of(ring, distance) + sub * sub_rows, sub_rows)
        there = full_ref.at[which, pl.ds(start, sub_rows), :]
        return pltpu.make_async_remote_copy(
            src_ref=there if src is None else src,
            dst_ref=there,
            send_sem=send_sem,
            recv_sem=recv_sem.at[ring, index],
            device_id={"tp": following(ring)},
            device_id_type=pl.DeviceIdType.MESH,
        )

    for sub in range(SUBS):
        for ring in range(RINGS):
            own = dy_ref.at[pl.ds(ring * piece + sub * sub_rows, sub_rows), :]
            message(ring, own, 0, 0, sub, sub).start()

    mine = pl.ds(pl.multiple_of(me * rows, rows), rows)
    bounce = [blk.at[pl.ds(i * rows, rows), :] for i in range(2)]
    for i, ref in enumerate((dy_ref, x_ref)):
        pltpu.make_async_copy(ref, bounce[i], wd_sem.at[i]).start()
    for i, ref in enumerate((dy_ref, x_ref)):
        pltpu.make_async_copy(ref, bounce[i], wd_sem.at[i]).wait()
        pltpu.make_async_copy(bounce[i], full_ref.at[i, mine, :], wd_sem.at[i]).start()
    for i in range(2):
        pltpu.make_async_copy(bounce[i], full_ref.at[i, mine, :], wd_sem.at[i]).wait()

    def serve(index, carry=None):
        step, sub = index // SUBS + 1, index % SUBS
        for ring in range(RINGS):
            message(ring, None, (step - 1) // hops, (step - 1) % hops + 1, sub, index).wait_recv()

        @pl.when(step < 2 * hops)
        def _():
            for ring in range(RINGS):
                message(ring, None, step // hops, step % hops, sub, index + SUBS).start()

    def served_before(tile):
        first = (per_block - 1) * SUBS
        return first + tile * (messages - first) // (blocks * tiles)

    def serve_after(tile):
        lax.fori_loop(served_before(tile), served_before(tile + 1), lambda i, c: serve(i), None)

    def load_wd(j, slot):
        src = wd_ref.at[pl.ds(pl.multiple_of(j * tile_f, tile_f), tile_f), :]
        return pltpu.make_async_copy(src, wd_buf.at[slot], wd_sem.at[slot])

    def load_w2(j, slot):
        at = pl.ds(pl.multiple_of(j * tile_d, tile_d), tile_d)
        return [
            pltpu.make_async_copy(ref.at[at, :], w2_buf.at[slot, i], w2_sem.at[slot, i])
            for i, ref in enumerate((wg_ref, wu_ref))
        ]

    def pieces(block, body):
        def by_distance(i, carry):
            for ring in range(RINGS):
                body(
                    rows_of(ring, block * per_block + i),
                    pl.multiple_of(i * rows + ring * piece, piece),
                )

        lax.fori_loop(0, per_block, by_distance, None)

    load_wd(0, 0).start()
    lax.fori_loop(0, (per_block - 1) * SUBS, lambda i, c: serve(i), None)

    def one_block(block, carry):
        for c in load_w2(0, 0):
            c.start()

        def fetch(there, here):
            pltpu.make_async_copy(full_ref.at[0, pl.ds(there, piece), :], blk.at[pl.ds(here, piece), :], blk_sem).start()
            for i, ref in enumerate((gate_ref, up_ref)):
                pltpu.make_async_copy(
                    ref.at[pl.ds(there, piece), :], gu_buf.at[i, pl.ds(here, piece), :], gu_sem.at[i]
                ).start()

        pieces(block, fetch)
        pltpu.make_async_copy(full_ref.at[0, pl.ds(0, blk.shape[0]), :], blk, blk_sem).wait()
        for i, ref in enumerate((gate_ref, up_ref)):
            pltpu.make_async_copy(ref.at[pl.ds(0, blk.shape[0]), :], gu_buf.at[i], gu_sem.at[i]).wait()

        def tile_a_body(j, carry):
            slot = j % 2
            load_wd(j, slot).wait()

            @pl.when(j + 1 < tiles_a)
            def _():
                load_wd(j + 1, 1 - slot).start()

            dh_buf[...] = lax.dot_general(blk[...], wd_buf[slot], NT, preferred_element_type=F32)
            cols = pl.ds(pl.multiple_of(j * tile_f, tile_f), tile_f)
            chunk = 32

            def elementwise(i, c):
                at = pl.ds(pl.multiple_of(i * chunk, chunk), chunk)
                h, dgate, dup = act_grads(
                    gu_buf[0, at, cols].astype(F32), gu_buf[1, at, cols].astype(F32), dh_buf[at, :]
                )
                grads[0, at, cols] = dgate.astype(BF16)
                grads[1, at, cols] = dup.astype(BF16)
                grads[2, at, cols] = h.astype(BF16)

            lax.fori_loop(0, blk.shape[0] // chunk, elementwise, None)
            serve_after(block * tiles + j)

        lax.fori_loop(0, tiles_a, tile_a_body, None)

        def put_grads(there, here):
            for i, ref in enumerate((dg_ref, du_ref, hid_ref)):
                pltpu.make_async_copy(
                    grads.at[i, pl.ds(here, piece), :], ref.at[pl.ds(there, piece), :], grads_sem.at[i]
                ).start()

        pieces(block, put_grads)

        @pl.when(block + 1 < blocks)
        def _():
            load_wd(0, 0).start()

        def wait_out(slot):
            pltpu.make_async_copy(
                obuf.at[slot], dx_ref.at[pl.ds(0, blk.shape[0]), pl.ds(0, tile_d)], o_sem.at[slot]
            ).wait()

        def tile_b_body(j, carry):
            slot = j % 2
            for c in load_w2(j, slot):
                c.wait()

            @pl.when(j + 1 < tiles_b)
            def _():
                for c in load_w2(j + 1, 1 - slot):
                    c.start()

            @pl.when(j >= 2)
            def _():
                wait_out(slot)

            obuf[slot] = (
                lax.dot_general(grads[0], w2_buf[slot, 0], NT, preferred_element_type=F32)
                + lax.dot_general(grads[1], w2_buf[slot, 1], NT, preferred_element_type=F32)
            ).astype(BF16)
            cols = pl.ds(pl.multiple_of(j * tile_d, tile_d), tile_d)

            def put(there, here):
                pltpu.make_async_copy(
                    obuf.at[slot, pl.ds(here, piece), :], dx_ref.at[pl.ds(there, piece), cols], o_sem.at[slot]
                ).start()

            pieces(block, put)
            serve_after(block * tiles + tiles_a + j)

        lax.fori_loop(0, tiles_b, tile_b_body, None)
        for slot in range(2):
            wait_out(slot)
        for i, ref in enumerate((dg_ref, du_ref, hid_ref)):
            pltpu.make_async_copy(grads.at[i], ref.at[pl.ds(0, blk.shape[0]), :], grads_sem.at[i]).wait()

    lax.fori_loop(0, blocks, one_block, None)
    sent = full_ref.at[:, pl.ds(0, hops * rows), :]
    pltpu.make_async_copy(sent, sent, send_sem).wait()


def gather(mesh, x, dy, gate, up, w_gate, w_up, w_down, tile_f=256, tile_d=512, block=512):
    n = mesh.shape["tp"]
    rows, d_model = x.shape
    total, ff = gate.shape
    tile_f, tile_d, block = min(tile_f, ff), min(tile_d, d_model), min(block, total)
    hbm = pl.BlockSpec(memory_space=pl.ANY)
    kept = jax.ShapeDtypeStruct((total, ff), BF16)
    messages = 2 * (n - 1) * SUBS
    return pl.pallas_call(
        functools.partial(gather_kernel, n, tile_f, tile_d),
        name="gather",
        out_shape=(
            jax.ShapeDtypeStruct((2, total, d_model), BF16),
            kept, kept, kept,
            jax.ShapeDtypeStruct((total, d_model), BF16),
        ),
        in_specs=[hbm] * 7,
        out_specs=(hbm,) * 5,
        scratch_shapes=[
            pltpu.VMEM((block, d_model), BF16),
            pltpu.VMEM((2, tile_f, d_model), BF16),
            pltpu.VMEM((2, 2, tile_d, ff), BF16),
            pltpu.VMEM((2, block, ff), BF16),
            pltpu.VMEM((block, tile_f), F32),
            pltpu.VMEM((3, block, ff), BF16),
            pltpu.VMEM((2, block, tile_d), BF16),
            pltpu.SemaphoreType.DMA,
            pltpu.SemaphoreType.DMA((RINGS, messages)),
            pltpu.SemaphoreType.DMA,
            pltpu.SemaphoreType.DMA((2,)),
            pltpu.SemaphoreType.DMA((2, 2)),
            pltpu.SemaphoreType.DMA((2,)),
            pltpu.SemaphoreType.DMA((3,)),
            pltpu.SemaphoreType.DMA((2,)),
        ],
        compiler_params=pltpu.CompilerParams(collective_id=0, has_side_effects=True, vmem_limit_bytes=58 * 2**20),
        cost_estimate=pl.CostEstimate(
            flops=6 * total * d_model * ff, bytes_accessed=2 * 4 * 3 * ff * d_model, transcendentals=total * ff
        ),
    )(x, dy, gate, up, w_gate, w_up, w_down)


def solution(mesh):
    rows = P(("dp", "tp"), None)
    both = P("dp", "tp")
    cols = P(None, "tp")

    def body(x, dy, gate, up, w_gate, w_up, w_down):
        full, d_gate, d_up, hidden, dx = gather(mesh, x, dy, gate, up, w_gate, w_up, w_down)
        dx = lax.psum_scatter(dx, "tp", scatter_dimension=0, tiled=True)

        def dw(a, b):
            return lax.dot_general(a, b, TN, preferred_element_type=F32).astype(BF16)

        return dx, dw(full[1], d_gate), dw(full[1], d_up), dw(hidden, full[0])

    return jax.shard_map(
        body,
        mesh=mesh,
        in_specs=(rows, rows, both, both, cols, cols, P("tp", None)),
        out_specs=(rows, both, both, rows),
        check_vma=False,
    )
```

```python
import functools
import math

import jax
import jax.numpy as jnp
from jax import lax
from jax.experimental import pallas as pl
from jax.experimental.pallas import tpu as pltpu
from jax.sharding import PartitionSpec as P

RINGS = 4
SUBS = 4
LATE = 3
FETCH = 2
TILE_A = 2
BF16 = jnp.bfloat16
F32 = jnp.float32
NT = (((1,), (1,)), ((), ()))
TN = (((0,), (0,)), ((), ()))


def act_grads(g, u, dh):
    sig = jax.nn.sigmoid(g)
    silu = g * sig
    ds = dh * u
    return silu * u, ds * (sig + silu * (1.0 - sig)), dh * silu


class Ring:
    def __init__(self, n, rows, full_ref, send_sem, recv_sem):
        self.n, self.rows, self.full_ref, self.send_sem, self.recv_sem = n, rows, full_ref, send_sem, recv_sem
        self.side = math.isqrt(n)
        self.hops = n - 1
        self.piece = rows // RINGS
        self.sub_rows = self.piece // SUBS
        self.me = lax.axis_index("tp")
        a, b = self.me // self.side, self.me % self.side
        self.place = (a * self.side + (a + b) % self.side, b * self.side + (a + b) % self.side)

    def owner(self, r, distance):
        k = self.place[r // 2] - distance if r % 2 == 0 else self.place[r // 2] + distance
        k = (k + 2 * self.n) % self.n
        u = k // self.side
        v = (k - u) % self.side
        return u * self.side + v if r // 2 == 0 else v * self.side + u

    def following(self, r):
        return {"tp": self.owner(r, -1)}

    def rows_of(self, r, distance):
        return pl.multiple_of(self.owner(r, distance) * self.rows + r * self.piece, self.piece)

    def greet(self):
        barrier = pltpu.get_barrier_semaphore()
        for r in range(RINGS):
            pl.semaphore_signal(barrier, inc=1, device_id=self.following(r), device_id_type=pl.DeviceIdType.MESH)
        pl.semaphore_wait(barrier, RINGS)

    def message(self, r, step, sub, slot, src=None):
        start = pl.multiple_of(self.rows_of(r, step % self.hops) + sub * self.sub_rows, self.sub_rows)
        there = self.full_ref.at[step // self.hops, pl.ds(start, self.sub_rows), :]
        return pltpu.make_async_remote_copy(
            src_ref=there if src is None else src,
            dst_ref=there,
            send_sem=self.send_sem,
            recv_sem=self.recv_sem.at[r, slot],
            device_id=self.following(r),
            device_id_type=pl.DeviceIdType.MESH,
        )

    def arrival(self, r, step, sub, slot):
        start = pl.multiple_of(self.rows_of(r, (step - 1) % self.hops + 1) + sub * self.sub_rows, self.sub_rows)
        there = self.full_ref.at[(step - 1) // self.hops, pl.ds(start, self.sub_rows), :]
        return pltpu.make_async_remote_copy(
            src_ref=there,
            dst_ref=there,
            send_sem=self.send_sem,
            recv_sem=self.recv_sem.at[r, slot],
            device_id=self.following(r),
            device_id_type=pl.DeviceIdType.MESH,
        )

    def serve(self, index, slot, stop):
        step, sub = index // SUBS + 1, index % SUBS
        for r in range(RINGS):
            self.arrival(r, step, sub, slot).wait_recv()

        @pl.when(index + SUBS < stop)
        def _():
            for r in range(RINGS):
                self.message(r, step, sub, slot + SUBS).start()

    def sent(self, messages):
        whole = self.full_ref.at[:, pl.ds(0, messages // SUBS * self.rows // 2), :]
        pltpu.make_async_copy(whole, whole, self.send_sem).wait()


def gather_kernel(
    n, tile_f, tile_d,
    x_ref, dy_ref, gate_ref, up_ref, wg_ref, wu_ref, wd_ref,
    full_ref, dg_ref, du_ref, hid_ref, dx_ref,
    blk, wd_buf, w2_buf, gu_buf, dh_buf, grads, obuf,
    send_sem, recv_sem, blk_sem, wd_sem, w2_sem, gu_sem, grads_sem, o_sem,
):
    side = math.isqrt(n)
    rows, d_model = x_ref.shape
    ff = gate_ref.shape[1]
    piece = rows // RINGS
    sub_rows = piece // SUBS
    hops = n - 1
    per_block = blk.shape[0] // rows
    blocks = n // per_block
    tiles_a = ff // tile_f
    tiles_b = d_model // tile_d
    messages = (2 * hops - LATE) * SUBS

    ring = Ring(n, x_ref.shape[0], full_ref, send_sem, recv_sem)
    me = ring.me
    rows_of = ring.rows_of

    ring.greet()
    for sub in range(SUBS):
        for r in range(RINGS):
            own = dy_ref.at[pl.ds(r * piece + sub * sub_rows, sub_rows), :]
            ring.message(r, 0, sub, sub, own).start()

    mine = pl.ds(pl.multiple_of(me * rows, rows), rows)
    bounce = [blk.at[pl.ds(i * rows, rows), :] for i in range(2)]
    for i, ref in enumerate((dy_ref, x_ref)):
        pltpu.make_async_copy(ref, bounce[i], wd_sem.at[i]).start()
    for i, ref in enumerate((dy_ref, x_ref)):
        pltpu.make_async_copy(ref, bounce[i], wd_sem.at[i]).wait()
        pltpu.make_async_copy(bounce[i], full_ref.at[i, mine, :], wd_sem.at[i]).start()
    for i in range(2):
        pltpu.make_async_copy(bounce[i], full_ref.at[i, mine, :], wd_sem.at[i]).wait()

    def serve(index):
        ring.serve(index, index, messages)

    units = FETCH + TILE_A * tiles_a + tiles_b
    first = (per_block - 1) * SUBS

    def serve_between(block, since, until):
        def served(unit):
            return first + (block * units + unit) * (messages - first) // (blocks * units)

        lax.fori_loop(served(since), served(until), lambda i, c: serve(i), None)

    def load_wd(j, slot):
        src = wd_ref.at[pl.ds(pl.multiple_of(j * tile_f, tile_f), tile_f), :]
        return pltpu.make_async_copy(src, wd_buf.at[slot], wd_sem.at[slot])

    def load_w2(j, slot):
        at = pl.ds(pl.multiple_of(j * tile_d, tile_d), tile_d)
        return [
            pltpu.make_async_copy(ref.at[at, :], w2_buf.at[slot, i], w2_sem.at[slot, i])
            for i, ref in enumerate((wg_ref, wu_ref))
        ]

    def pieces(block, body):
        def by_distance(i, carry):
            for r in range(RINGS):
                body(
                    rows_of(r, block * per_block + i),
                    pl.multiple_of(i * rows + r * piece, piece),
                )

        lax.fori_loop(0, per_block, by_distance, None)

    load_wd(0, 0).start()
    lax.fori_loop(0, first, lambda i, c: serve(i), None)

    def one_block(block, carry):
        for c in load_w2(0, 0):
            c.start()

        def fetch(there, here):
            pltpu.make_async_copy(full_ref.at[0, pl.ds(there, piece), :], blk.at[pl.ds(here, piece), :], blk_sem).start()
            for i, ref in enumerate((gate_ref, up_ref)):
                pltpu.make_async_copy(
                    ref.at[pl.ds(there, piece), :], gu_buf.at[i, pl.ds(here, piece), :], gu_sem.at[i]
                ).start()

        pieces(block, fetch)
        serve_between(block, 0, FETCH)
        pltpu.make_async_copy(full_ref.at[0, pl.ds(0, blk.shape[0]), :], blk, blk_sem).wait()
        for i, ref in enumerate((gate_ref, up_ref)):
            pltpu.make_async_copy(ref.at[pl.ds(0, blk.shape[0]), :], gu_buf.at[i], gu_sem.at[i]).wait()

        def tile_a_body(j, carry):
            slot = j % 2
            load_wd(j, slot).wait()

            @pl.when(j + 1 < tiles_a)
            def _():
                load_wd(j + 1, 1 - slot).start()

            dh_buf[...] = lax.dot_general(blk[...], wd_buf[slot], NT, preferred_element_type=F32)
            cols = pl.ds(pl.multiple_of(j * tile_f, tile_f), tile_f)
            chunk = 32

            def elementwise(i, c):
                at = pl.ds(pl.multiple_of(i * chunk, chunk), chunk)
                h, dgate, dup = act_grads(
                    gu_buf[0, at, cols].astype(F32), gu_buf[1, at, cols].astype(F32), dh_buf[at, :]
                )
                grads[0, at, cols] = dgate.astype(BF16)
                grads[1, at, cols] = dup.astype(BF16)
                grads[2, at, cols] = h.astype(BF16)

            lax.fori_loop(0, blk.shape[0] // chunk, elementwise, None)
            serve_between(block, FETCH + TILE_A * j, FETCH + TILE_A * (j + 1))

        lax.fori_loop(0, tiles_a, tile_a_body, None)

        def put_grads(there, here):
            for i, ref in enumerate((dg_ref, du_ref, hid_ref)):
                pltpu.make_async_copy(
                    grads.at[i, pl.ds(here, piece), :], ref.at[pl.ds(there, piece), :], grads_sem.at[i]
                ).start()

        pieces(block, put_grads)

        @pl.when(block + 1 < blocks)
        def _():
            load_wd(0, 0).start()

        def wait_out(slot):
            pltpu.make_async_copy(
                obuf.at[slot], dx_ref.at[pl.ds(0, blk.shape[0]), pl.ds(0, tile_d)], o_sem.at[slot]
            ).wait()

        def tile_b_body(j, carry):
            slot = j % 2
            for c in load_w2(j, slot):
                c.wait()

            @pl.when(j + 1 < tiles_b)
            def _():
                for c in load_w2(j + 1, 1 - slot):
                    c.start()

            @pl.when(j >= 2)
            def _():
                wait_out(slot)

            obuf[slot] = (
                lax.dot_general(grads[0], w2_buf[slot, 0], NT, preferred_element_type=F32)
                + lax.dot_general(grads[1], w2_buf[slot, 1], NT, preferred_element_type=F32)
            ).astype(BF16)
            cols = pl.ds(pl.multiple_of(j * tile_d, tile_d), tile_d)

            def put(there, here):
                pltpu.make_async_copy(
                    obuf.at[slot, pl.ds(here, piece), :], dx_ref.at[pl.ds(there, piece), cols], o_sem.at[slot]
                ).start()

            pieces(block, put)
            done = FETCH + TILE_A * tiles_a + j
            serve_between(block, done, done + 1)

        lax.fori_loop(0, tiles_b, tile_b_body, None)
        for slot in range(2):
            wait_out(slot)
        for i, ref in enumerate((dg_ref, du_ref, hid_ref)):
            pltpu.make_async_copy(grads.at[i], ref.at[pl.ds(0, blk.shape[0]), :], grads_sem.at[i]).wait()

    lax.fori_loop(0, blocks, one_block, None)
    ring.sent(messages)


def gather(mesh, x, dy, gate, up, w_gate, w_up, w_down, tile_f=256, tile_d=512, block=512):
    n = mesh.shape["tp"]
    rows, d_model = x.shape
    total, ff = gate.shape
    tile_f, tile_d, block = min(tile_f, ff), min(tile_d, d_model), min(block, total)
    hbm = pl.BlockSpec(memory_space=pl.ANY)
    kept = jax.ShapeDtypeStruct((total, ff), BF16)
    messages = (2 * (n - 1) - LATE) * SUBS
    return pl.pallas_call(
        functools.partial(gather_kernel, n, tile_f, tile_d),
        name="gather",
        out_shape=(
            jax.ShapeDtypeStruct((2, total, d_model), BF16),
            kept, kept, kept,
            jax.ShapeDtypeStruct((total, d_model), BF16),
        ),
        in_specs=[hbm] * 7,
        out_specs=(hbm,) * 5,
        scratch_shapes=[
            pltpu.VMEM((block, d_model), BF16),
            pltpu.VMEM((2, tile_f, d_model), BF16),
            pltpu.VMEM((2, 2, tile_d, ff), BF16),
            pltpu.VMEM((2, block, ff), BF16),
            pltpu.VMEM((block, tile_f), F32),
            pltpu.VMEM((3, block, ff), BF16),
            pltpu.VMEM((2, block, tile_d), BF16),
            pltpu.SemaphoreType.DMA,
            pltpu.SemaphoreType.DMA((RINGS, messages)),
            pltpu.SemaphoreType.DMA,
            pltpu.SemaphoreType.DMA((2,)),
            pltpu.SemaphoreType.DMA((2, 2)),
            pltpu.SemaphoreType.DMA((2,)),
            pltpu.SemaphoreType.DMA((3,)),
            pltpu.SemaphoreType.DMA((2,)),
        ],
        compiler_params=pltpu.CompilerParams(collective_id=0, has_side_effects=True, vmem_limit_bytes=58 * 2**20),
        cost_estimate=pl.CostEstimate(
            flops=6 * total * d_model * ff, bytes_accessed=2 * 4 * 3 * ff * d_model, transcendentals=total * ff
        ),
    )(x, dy, gate, up, w_gate, w_up, w_down)


def late_kernel(
    n, tile_d,
    full_in_ref, hidden_ref,
    full_ref, dw_ref,
    hid, dy_buf, obuf,
    send_sem, recv_sem, hid_sem, dy_sem, o_sem,
):
    del full_in_ref
    total, d_model = full_ref.shape[1:]
    ff = hidden_ref.shape[1]
    tiles = d_model // tile_d
    ring = Ring(n, total // n, full_ref, send_sem, recv_sem)
    stop = 2 * ring.hops * SUBS
    messages = LATE * SUBS
    first = stop - messages

    load = pltpu.make_async_copy(hidden_ref, hid, hid_sem)
    load.start()

    def load_dy(j, slot):
        at = pl.ds(pl.multiple_of(j * tile_d, tile_d), tile_d)
        return pltpu.make_async_copy(full_ref.at[0, :, at], dy_buf.at[slot], dy_sem.at[slot])

    def store(j, slot):
        at = pl.ds(pl.multiple_of(j * tile_d, tile_d), tile_d)
        return pltpu.make_async_copy(obuf.at[slot], dw_ref.at[:, at], o_sem.at[slot])

    load_dy(0, 0).start()
    ring.greet()
    for sub in range(SUBS):
        for r in range(RINGS):
            ring.message(r, first // SUBS, sub, sub).start()
    load.wait()

    def tile(j, carry):
        slot = j % 2
        load_dy(j, slot).wait()

        @pl.when(j + 1 < tiles)
        def _():
            load_dy(j + 1, 1 - slot).start()

        @pl.when(j >= 2)
        def _():
            store(j - 2, slot).wait()

        obuf[slot] = lax.dot_general(hid[...], dy_buf[slot], TN, preferred_element_type=F32).astype(BF16)
        store(j, slot).start()
        lax.fori_loop(
            j * messages // tiles,
            (j + 1) * messages // tiles,
            lambda i, c: ring.serve(first + i, i, stop),
            None,
        )

    lax.fori_loop(0, tiles, tile, None)
    for j in (tiles - 2, tiles - 1):
        store(j, j % 2).wait()
    ring.sent(messages)


def finish(mesh, full, hidden, tile_d=256):
    n = mesh.shape["tp"]
    _, total, d_model = full.shape
    ff = hidden.shape[1]
    hbm = pl.BlockSpec(memory_space=pl.ANY)
    return pl.pallas_call(
        functools.partial(late_kernel, n, tile_d),
        name="finish",
        out_shape=(jax.ShapeDtypeStruct(full.shape, BF16), jax.ShapeDtypeStruct((ff, d_model), BF16)),
        in_specs=[hbm] * 2,
        out_specs=(hbm,) * 2,
        input_output_aliases={0: 0},
        scratch_shapes=[
            pltpu.VMEM((total, ff), BF16),
            pltpu.VMEM((2, total, tile_d), BF16),
            pltpu.VMEM((2, ff, tile_d), BF16),
            pltpu.SemaphoreType.DMA,
            pltpu.SemaphoreType.DMA((RINGS, LATE * SUBS)),
            pltpu.SemaphoreType.DMA,
            pltpu.SemaphoreType.DMA((2,)),
            pltpu.SemaphoreType.DMA((2,)),
        ],
        compiler_params=pltpu.CompilerParams(collective_id=1, has_side_effects=True, vmem_limit_bytes=60 * 2**20),
        cost_estimate=pl.CostEstimate(
            flops=2 * total * d_model * ff, bytes_accessed=2 * (total * ff + total * d_model + ff * d_model), transcendentals=0
        ),
    )(full, hidden)


def copy_kernel(src_ref, out_ref):
    out_ref[...] = src_ref[...]


def copied(a, rows=256):
    spec = pl.BlockSpec((rows, a.shape[1]), lambda i: (i, 0))
    return pl.pallas_call(
        copy_kernel,
        name="copied",
        grid=(a.shape[0] // rows,),
        out_shape=jax.ShapeDtypeStruct(a.shape, a.dtype),
        in_specs=[spec],
        out_specs=spec,
        compiler_params=pltpu.CompilerParams(vmem_limit_bytes=40 * 2**20),
        cost_estimate=pl.CostEstimate(flops=a.size, bytes_accessed=4 * a.size, transcendentals=0),
    )(a)


def solution(mesh):
    rows = P(("dp", "tp"), None)
    both = P("dp", "tp")
    cols = P(None, "tp")

    def body(x, dy, gate, up, w_gate, w_up, w_down):
        full, d_gate, d_up, hidden, dx = gather(mesh, x, dy, gate, up, w_gate, w_up, w_down)
        dx = lax.psum_scatter(dx, "tp", scatter_dimension=0, tiled=True)
        full, dw_down = finish(mesh, full, hidden)

        def dw(a, b):
            return lax.dot_general(a, b, TN, preferred_element_type=F32).astype(BF16)

        return dx, dw(full[1], d_gate), dw(full[1], d_up), copied(dw_down)

    return jax.shard_map(
        body,
        mesh=mesh,
        in_specs=(rows, rows, both, both, cols, cols, P("tp", None)),
        out_specs=(rows, both, both, rows),
        check_vma=False,
    )
```

```python
import functools
import math

import jax
import jax.numpy as jnp
from jax import lax
from jax.experimental import pallas as pl
from jax.experimental.pallas import tpu as pltpu
from jax.sharding import PartitionSpec as P

RINGS = 4
SUBS = 4
LATE = 2
FETCH = 2
TILE_A = 2
TAIL = 8
BF16 = jnp.bfloat16
F32 = jnp.float32
NT = (((1,), (1,)), ((), ()))
TN = (((0,), (0,)), ((), ()))


def act_grads(g, u, dh):
    sig = jax.nn.sigmoid(g)
    silu = g * sig
    ds = dh * u
    return silu * u, ds * (sig + silu * (1.0 - sig)), dh * silu


class Ring:
    def __init__(self, n, rows, full_ref, send_sem, recv_sem):
        self.n, self.rows, self.full_ref, self.send_sem, self.recv_sem = n, rows, full_ref, send_sem, recv_sem
        self.side = math.isqrt(n)
        self.hops = n - 1
        self.piece = rows // RINGS
        self.sub_rows = self.piece // SUBS
        self.me = lax.axis_index("tp")
        a, b = self.me // self.side, self.me % self.side
        self.place = (a * self.side + (a + b) % self.side, b * self.side + (a + b) % self.side)

    def owner(self, r, distance):
        k = self.place[r // 2] - distance if r % 2 == 0 else self.place[r // 2] + distance
        k = (k + 2 * self.n) % self.n
        u = k // self.side
        v = (k - u) % self.side
        return u * self.side + v if r // 2 == 0 else v * self.side + u

    def following(self, r):
        return {"tp": self.owner(r, -1)}

    def rows_of(self, r, distance):
        return pl.multiple_of(self.owner(r, distance) * self.rows + r * self.piece, self.piece)

    def greet(self):
        barrier = pltpu.get_barrier_semaphore()
        for r in range(RINGS):
            pl.semaphore_signal(barrier, inc=1, device_id=self.following(r), device_id_type=pl.DeviceIdType.MESH)
        pl.semaphore_wait(barrier, RINGS)

    def message(self, r, step, sub, slot, src=None):
        start = pl.multiple_of(self.rows_of(r, step % self.hops) + sub * self.sub_rows, self.sub_rows)
        there = self.full_ref.at[step // self.hops, pl.ds(start, self.sub_rows), :]
        return pltpu.make_async_remote_copy(
            src_ref=there if src is None else src,
            dst_ref=there,
            send_sem=self.send_sem,
            recv_sem=self.recv_sem.at[r, slot],
            device_id=self.following(r),
            device_id_type=pl.DeviceIdType.MESH,
        )

    def arrival(self, r, step, sub, slot):
        start = pl.multiple_of(self.rows_of(r, (step - 1) % self.hops + 1) + sub * self.sub_rows, self.sub_rows)
        there = self.full_ref.at[(step - 1) // self.hops, pl.ds(start, self.sub_rows), :]
        return pltpu.make_async_remote_copy(
            src_ref=there,
            dst_ref=there,
            send_sem=self.send_sem,
            recv_sem=self.recv_sem.at[r, slot],
            device_id=self.following(r),
            device_id_type=pl.DeviceIdType.MESH,
        )

    def serve(self, index, slot, stop):
        step, sub = index // SUBS + 1, index % SUBS
        for r in range(RINGS):
            self.arrival(r, step, sub, slot).wait_recv()

        @pl.when(index + SUBS < stop)
        def _():
            for r in range(RINGS):
                self.message(r, step, sub, slot + SUBS).start()

    def sent(self, messages):
        whole = self.full_ref.at[:, pl.ds(0, messages // SUBS * self.rows // 2), :]
        pltpu.make_async_copy(whole, whole, self.send_sem).wait()


def gather_kernel(
    n, tile_f, tile_d,
    x_ref, dy_ref, gate_ref, up_ref, wg_ref, wu_ref, wd_ref,
    full_ref, dg_ref, du_ref, hid_ref, dx_ref,
    blk, wd_buf, w2_buf, gu_buf, dh_buf, grads, obuf,
    send_sem, recv_sem, blk_sem, wd_sem, w2_sem, gu_sem, grads_sem, o_sem,
):
    side = math.isqrt(n)
    rows, d_model = x_ref.shape
    ff = gate_ref.shape[1]
    piece = rows // RINGS
    sub_rows = piece // SUBS
    hops = n - 1
    per_block = blk.shape[0] // rows
    blocks = n // per_block
    tiles_a = ff // tile_f
    tiles_b = d_model // tile_d
    messages = (2 * hops - LATE) * SUBS

    ring = Ring(n, x_ref.shape[0], full_ref, send_sem, recv_sem)
    me = ring.me
    rows_of = ring.rows_of

    ring.greet()
    for sub in range(SUBS):
        for r in range(RINGS):
            own = dy_ref.at[pl.ds(r * piece + sub * sub_rows, sub_rows), :]
            ring.message(r, 0, sub, sub, own).start()

    mine = pl.ds(pl.multiple_of(me * rows, rows), rows)
    bounce = [blk.at[pl.ds(i * rows, rows), :] for i in range(2)]
    for i, ref in enumerate((dy_ref, x_ref)):
        pltpu.make_async_copy(ref, bounce[i], wd_sem.at[i]).start()
    for i, ref in enumerate((dy_ref, x_ref)):
        pltpu.make_async_copy(ref, bounce[i], wd_sem.at[i]).wait()
        pltpu.make_async_copy(bounce[i], full_ref.at[i, mine, :], wd_sem.at[i]).start()
    for i in range(2):
        pltpu.make_async_copy(bounce[i], full_ref.at[i, mine, :], wd_sem.at[i]).wait()

    def serve(index):
        ring.serve(index, index, messages)

    units = FETCH + TILE_A * tiles_a + tiles_b
    first = (per_block - 1) * SUBS
    paced = messages - TAIL

    def serve_between(block, since, until):
        def served(unit):
            return first + (block * units + unit) * (paced - first) // (blocks * units)

        lax.fori_loop(served(since), served(until), lambda i, c: serve(i), None)

    def load_wd(j, slot):
        src = wd_ref.at[pl.ds(pl.multiple_of(j * tile_f, tile_f), tile_f), :]
        return pltpu.make_async_copy(src, wd_buf.at[slot], wd_sem.at[slot])

    def load_w2(j, slot):
        at = pl.ds(pl.multiple_of(j * tile_d, tile_d), tile_d)
        return [
            pltpu.make_async_copy(ref.at[at, :], w2_buf.at[slot, i], w2_sem.at[slot, i])
            for i, ref in enumerate((wg_ref, wu_ref))
        ]

    def pieces(block, body):
        def by_distance(i, carry):
            for r in range(RINGS):
                body(
                    rows_of(r, block * per_block + i),
                    pl.multiple_of(i * rows + r * piece, piece),
                )

        lax.fori_loop(0, per_block, by_distance, None)

    load_wd(0, 0).start()
    lax.fori_loop(0, first, lambda i, c: serve(i), None)

    def one_block(block, carry):
        for c in load_w2(0, 0):
            c.start()

        def fetch(there, here):
            pltpu.make_async_copy(full_ref.at[0, pl.ds(there, piece), :], blk.at[pl.ds(here, piece), :], blk_sem).start()
            for i, ref in enumerate((gate_ref, up_ref)):
                pltpu.make_async_copy(
                    ref.at[pl.ds(there, piece), :], gu_buf.at[i, pl.ds(here, piece), :], gu_sem.at[i]
                ).start()

        pieces(block, fetch)
        serve_between(block, 0, FETCH)
        pltpu.make_async_copy(full_ref.at[0, pl.ds(0, blk.shape[0]), :], blk, blk_sem).wait()
        for i, ref in enumerate((gate_ref, up_ref)):
            pltpu.make_async_copy(ref.at[pl.ds(0, blk.shape[0]), :], gu_buf.at[i], gu_sem.at[i]).wait()

        def tile_a_body(j, carry):
            slot = j % 2
            load_wd(j, slot).wait()

            @pl.when(j + 1 < tiles_a)
            def _():
                load_wd(j + 1, 1 - slot).start()

            dh_buf[...] = lax.dot_general(blk[...], wd_buf[slot], NT, preferred_element_type=F32)
            cols = pl.ds(pl.multiple_of(j * tile_f, tile_f), tile_f)
            chunk = 32

            def elementwise(i, c):
                at = pl.ds(pl.multiple_of(i * chunk, chunk), chunk)
                h, dgate, dup = act_grads(
                    gu_buf[0, at, cols].astype(F32), gu_buf[1, at, cols].astype(F32), dh_buf[at, :]
                )
                grads[0, at, cols] = dgate.astype(BF16)
                grads[1, at, cols] = dup.astype(BF16)
                grads[2, at, cols] = h.astype(BF16)

            lax.fori_loop(0, blk.shape[0] // chunk, elementwise, None)
            serve_between(block, FETCH + TILE_A * j, FETCH + TILE_A * (j + 1))

        lax.fori_loop(0, tiles_a, tile_a_body, None)

        def put_grads(there, here):
            for i, ref in enumerate((dg_ref, du_ref, hid_ref)):
                pltpu.make_async_copy(
                    grads.at[i, pl.ds(here, piece), :], ref.at[pl.ds(there, piece), :], grads_sem.at[i]
                ).start()

        pieces(block, put_grads)

        @pl.when(block + 1 < blocks)
        def _():
            load_wd(0, 0).start()

        def wait_out(slot):
            pltpu.make_async_copy(
                obuf.at[slot], dx_ref.at[pl.ds(0, blk.shape[0]), pl.ds(0, tile_d)], o_sem.at[slot]
            ).wait()

        def tile_b_body(j, carry):
            slot = j % 2
            for c in load_w2(j, slot):
                c.wait()

            @pl.when(j + 1 < tiles_b)
            def _():
                for c in load_w2(j + 1, 1 - slot):
                    c.start()

            @pl.when(j >= 2)
            def _():
                wait_out(slot)

            obuf[slot] = (
                lax.dot_general(grads[0], w2_buf[slot, 0], NT, preferred_element_type=F32)
                + lax.dot_general(grads[1], w2_buf[slot, 1], NT, preferred_element_type=F32)
            ).astype(BF16)
            cols = pl.ds(pl.multiple_of(j * tile_d, tile_d), tile_d)

            def put(there, here):
                pltpu.make_async_copy(
                    obuf.at[slot, pl.ds(here, piece), :], dx_ref.at[pl.ds(there, piece), cols], o_sem.at[slot]
                ).start()

            pieces(block, put)
            done = FETCH + TILE_A * tiles_a + j
            serve_between(block, done, done + 1)

        lax.fori_loop(0, tiles_b, tile_b_body, None)
        for slot in range(2):
            wait_out(slot)
        for i, ref in enumerate((dg_ref, du_ref, hid_ref)):
            pltpu.make_async_copy(grads.at[i], ref.at[pl.ds(0, blk.shape[0]), :], grads_sem.at[i]).wait()

    assert all(first + b * (paced - first) // blocks >= ((b + 1) * per_block - 1) * SUBS for b in range(blocks))
    lax.fori_loop(0, blocks, one_block, None)
    lax.fori_loop(paced, messages, lambda i, c: serve(i), None)
    ring.sent(messages)


def gather(mesh, x, dy, gate, up, w_gate, w_up, w_down, tile_f=256, tile_d=512, block=512):
    n = mesh.shape["tp"]
    rows, d_model = x.shape
    total, ff = gate.shape
    tile_f, tile_d, block = min(tile_f, ff), min(tile_d, d_model), min(block, total)
    hbm = pl.BlockSpec(memory_space=pl.ANY)
    kept = jax.ShapeDtypeStruct((total, ff), BF16)
    messages = (2 * (n - 1) - LATE) * SUBS
    return pl.pallas_call(
        functools.partial(gather_kernel, n, tile_f, tile_d),
        name="gather",
        out_shape=(
            jax.ShapeDtypeStruct((2, total, d_model), BF16),
            kept, kept, kept,
            jax.ShapeDtypeStruct((total, d_model), BF16),
        ),
        in_specs=[hbm] * 7,
        out_specs=(hbm,) * 5,
        scratch_shapes=[
            pltpu.VMEM((block, d_model), BF16),
            pltpu.VMEM((2, tile_f, d_model), BF16),
            pltpu.VMEM((2, 2, tile_d, ff), BF16),
            pltpu.VMEM((2, block, ff), BF16),
            pltpu.VMEM((block, tile_f), F32),
            pltpu.VMEM((3, block, ff), BF16),
            pltpu.VMEM((2, block, tile_d), BF16),
            pltpu.SemaphoreType.DMA,
            pltpu.SemaphoreType.DMA((RINGS, messages)),
            pltpu.SemaphoreType.DMA,
            pltpu.SemaphoreType.DMA((2,)),
            pltpu.SemaphoreType.DMA((2, 2)),
            pltpu.SemaphoreType.DMA((2,)),
            pltpu.SemaphoreType.DMA((3,)),
            pltpu.SemaphoreType.DMA((2,)),
        ],
        compiler_params=pltpu.CompilerParams(collective_id=0, has_side_effects=True, vmem_limit_bytes=58 * 2**20),
        cost_estimate=pl.CostEstimate(
            flops=6 * total * d_model * ff, bytes_accessed=2 * 4 * 3 * ff * d_model, transcendentals=total * ff
        ),
    )(x, dy, gate, up, w_gate, w_up, w_down)


def late_kernel(
    n, tile_d,
    full_in_ref, hidden_ref,
    full_ref, dw_ref,
    hid, dy_buf, obuf,
    send_sem, recv_sem, hid_sem, dy_sem, o_sem,
):
    del full_in_ref
    total, d_model = full_ref.shape[1:]
    ff = hidden_ref.shape[1]
    tiles = d_model // tile_d
    ring = Ring(n, total // n, full_ref, send_sem, recv_sem)
    stop = 2 * ring.hops * SUBS
    messages = LATE * SUBS
    first = stop - messages

    ring.greet()
    for sub in range(SUBS):
        for r in range(RINGS):
            ring.message(r, first // SUBS, sub, sub).start()

    load = pltpu.make_async_copy(hidden_ref, hid, hid_sem)
    load.start()

    def load_dy(j, slot):
        at = pl.ds(pl.multiple_of(j * tile_d, tile_d), tile_d)
        return pltpu.make_async_copy(full_ref.at[0, :, at], dy_buf.at[slot], dy_sem.at[slot])

    def store(j, slot):
        at = pl.ds(pl.multiple_of(j * tile_d, tile_d), tile_d)
        return pltpu.make_async_copy(obuf.at[slot], dw_ref.at[:, at], o_sem.at[slot])

    load_dy(0, 0).start()
    load.wait()

    def tile(j, carry):
        slot = j % 2
        load_dy(j, slot).wait()

        @pl.when(j + 1 < tiles)
        def _():
            load_dy(j + 1, 1 - slot).start()

        @pl.when(j >= 2)
        def _():
            store(j - 2, slot).wait()

        obuf[slot] = lax.dot_general(hid[...], dy_buf[slot], TN, preferred_element_type=F32).astype(BF16)
        store(j, slot).start()
        lax.fori_loop(
            j * messages // tiles,
            (j + 1) * messages // tiles,
            lambda i, c: ring.serve(first + i, i, stop),
            None,
        )

    lax.fori_loop(0, tiles, tile, None)
    for j in (tiles - 2, tiles - 1):
        store(j, j % 2).wait()
    ring.sent(messages)


def finish(mesh, full, hidden, tile_d=256):
    n = mesh.shape["tp"]
    _, total, d_model = full.shape
    ff = hidden.shape[1]
    hbm = pl.BlockSpec(memory_space=pl.ANY)
    return pl.pallas_call(
        functools.partial(late_kernel, n, tile_d),
        name="finish",
        out_shape=(jax.ShapeDtypeStruct(full.shape, BF16), jax.ShapeDtypeStruct((ff, d_model), BF16)),
        in_specs=[hbm] * 2,
        out_specs=(hbm,) * 2,
        input_output_aliases={0: 0},
        scratch_shapes=[
            pltpu.VMEM((total, ff), BF16),
            pltpu.VMEM((2, total, tile_d), BF16),
            pltpu.VMEM((2, ff, tile_d), BF16),
            pltpu.SemaphoreType.DMA,
            pltpu.SemaphoreType.DMA((RINGS, LATE * SUBS)),
            pltpu.SemaphoreType.DMA,
            pltpu.SemaphoreType.DMA((2,)),
            pltpu.SemaphoreType.DMA((2,)),
        ],
        compiler_params=pltpu.CompilerParams(collective_id=1, has_side_effects=True, vmem_limit_bytes=60 * 2**20),
        cost_estimate=pl.CostEstimate(
            flops=2 * total * d_model * ff, bytes_accessed=2 * (total * ff + total * d_model + ff * d_model), transcendentals=0
        ),
    )(full, hidden)


def copy_kernel(src_ref, out_ref, buf, in_sem, out_sem):
    slots, rows, _ = buf.shape
    ahead = slots // 2
    chunks = src_ref.shape[0] // rows

    def chunk(ref, i):
        return ref.at[pl.ds(pl.multiple_of(i * rows, rows), rows), :]

    def load(i):
        return pltpu.make_async_copy(chunk(src_ref, i), buf.at[i % slots], in_sem.at[i % slots])

    def store(i):
        return pltpu.make_async_copy(buf.at[i % slots], chunk(out_ref, i), out_sem.at[i % slots])

    for i in range(ahead):
        load(i).start()

    def step(i, carry):
        load(i).wait()
        store(i).start()

        @pl.when(jnp.logical_and(i + ahead >= slots, i + ahead < chunks))
        def _():
            store(i + ahead - slots).wait()

        @pl.when(i + ahead < chunks)
        def _():
            load(i + ahead).start()

    lax.fori_loop(0, chunks, step, None)
    for i in range(chunks - slots, chunks):
        store(i).wait()


def copied(a, rows=64, slots=8):
    hbm = pl.BlockSpec(memory_space=pl.ANY)
    return pl.pallas_call(
        copy_kernel,
        name="copied",
        out_shape=jax.ShapeDtypeStruct(a.shape, a.dtype),
        in_specs=[hbm],
        out_specs=hbm,
        scratch_shapes=[
            pltpu.VMEM((slots, rows, a.shape[1]), a.dtype),
            pltpu.SemaphoreType.DMA((slots,)),
            pltpu.SemaphoreType.DMA((slots,)),
        ],
        compiler_params=pltpu.CompilerParams(vmem_limit_bytes=60 * 2**20),
        cost_estimate=pl.CostEstimate(flops=a.size, bytes_accessed=4 * a.size, transcendentals=0),
    )(a)


def solution(mesh):
    rows = P(("dp", "tp"), None)
    both = P("dp", "tp")
    cols = P(None, "tp")

    def body(x, dy, gate, up, w_gate, w_up, w_down):
        full, d_gate, d_up, hidden, dx = gather(mesh, x, dy, gate, up, w_gate, w_up, w_down)
        dx = lax.psum_scatter(dx, "tp", scatter_dimension=0, tiled=True)
        full, dw_down = finish(mesh, full, hidden)

        def dw(a, b):
            return lax.dot_general(a, b, TN, preferred_element_type=F32).astype(BF16)

        return dx, dw(full[1], d_gate), dw(full[1], d_up), copied(dw_down)

    return jax.shard_map(
        body,
        mesh=mesh,
        in_specs=(rows, rows, both, both, cols, cols, P("tp", None)),
        out_specs=(rows, both, both, rows),
        check_vma=False,
    )
```

```python
import functools
import math

import jax
import jax.numpy as jnp
from jax import lax
from jax.experimental import pallas as pl
from jax.experimental.pallas import tpu as pltpu
from jax.sharding import PartitionSpec as P

RINGS = 4
SUBS = 4
LATE = 3
FETCH = 2
TILE_A = 2
TAIL = 8
GROUP = 4
BF16 = jnp.bfloat16
F32 = jnp.float32
NT = (((1,), (1,)), ((), ()))
TN = (((0,), (0,)), ((), ()))


def act_grads(g, u, dh):
    sig = jax.nn.sigmoid(g)
    silu = g * sig
    ds = dh * u
    return silu * u, ds * (sig + silu * (1.0 - sig)), dh * silu


class Ring:
    def __init__(self, n, rows, full_ref, send_sem, recv_sem):
        self.n, self.rows, self.full_ref, self.send_sem, self.recv_sem = n, rows, full_ref, send_sem, recv_sem
        self.side = math.isqrt(n)
        self.hops = n - 1
        self.piece = rows // RINGS
        self.sub_rows = self.piece // SUBS
        self.me = lax.axis_index("tp")
        a, b = self.me // self.side, self.me % self.side
        self.place = (a * self.side + (a + b) % self.side, b * self.side + (a + b) % self.side)

    def owner(self, r, distance):
        k = self.place[r // 2] - distance if r % 2 == 0 else self.place[r // 2] + distance
        k = (k + 2 * self.n) % self.n
        u = k // self.side
        v = (k - u) % self.side
        return u * self.side + v if r // 2 == 0 else v * self.side + u

    def following(self, r):
        return {"tp": self.owner(r, -1)}

    def rows_of(self, r, distance):
        return pl.multiple_of(self.owner(r, distance) * self.rows + r * self.piece, self.piece)

    def greet(self):
        barrier = pltpu.get_barrier_semaphore()
        for r in range(RINGS):
            pl.semaphore_signal(barrier, inc=1, device_id=self.following(r), device_id_type=pl.DeviceIdType.MESH)
        pl.semaphore_wait(barrier, RINGS)

    def message(self, r, step, sub, slot, src=None):
        start = pl.multiple_of(self.rows_of(r, step % self.hops) + sub * self.sub_rows, self.sub_rows)
        there = self.full_ref.at[step // self.hops, pl.ds(start, self.sub_rows), :]
        return pltpu.make_async_remote_copy(
            src_ref=there if src is None else src,
            dst_ref=there,
            send_sem=self.send_sem,
            recv_sem=self.recv_sem.at[r, slot],
            device_id=self.following(r),
            device_id_type=pl.DeviceIdType.MESH,
        )

    def arrival(self, r, step, sub, slot):
        start = pl.multiple_of(self.rows_of(r, (step - 1) % self.hops + 1) + sub * self.sub_rows, self.sub_rows)
        there = self.full_ref.at[(step - 1) // self.hops, pl.ds(start, self.sub_rows), :]
        return pltpu.make_async_remote_copy(
            src_ref=there,
            dst_ref=there,
            send_sem=self.send_sem,
            recv_sem=self.recv_sem.at[r, slot],
            device_id=self.following(r),
            device_id_type=pl.DeviceIdType.MESH,
        )

    def serve(self, index, slot, stop):
        step, sub = index // SUBS + 1, index % SUBS
        for r in range(RINGS):
            self.arrival(r, step, sub, slot).wait_recv()

        @pl.when(index + SUBS < stop)
        def _():
            for r in range(RINGS):
                self.message(r, step, sub, slot + SUBS).start()

    def sent(self, messages):
        whole = self.full_ref.at[:, pl.ds(0, messages // SUBS * self.rows // 2), :]
        pltpu.make_async_copy(whole, whole, self.send_sem).wait()


def gather_kernel(
    n, tile_f, tile_d,
    x_ref, dy_ref, gate_ref, up_ref, wg_ref, wu_ref, wd_ref,
    full_ref, dg_ref, du_ref, hid_ref, dx_ref,
    blk, wd_buf, w2_buf, gu_buf, dh_buf, grads,
    send_sem, recv_sem, blk_sem, wd_sem, w2_sem, gu_sem, grads_sem, o_sem,
):
    side = math.isqrt(n)
    rows, d_model = x_ref.shape
    ff = gate_ref.shape[1]
    piece = rows // RINGS
    sub_rows = piece // SUBS
    hops = n - 1
    per_block = blk.shape[0] // rows
    blocks = n // per_block
    tiles_a = ff // tile_f
    tiles_b = d_model // tile_d
    messages = (2 * hops - LATE) * SUBS

    ring = Ring(n, x_ref.shape[0], full_ref, send_sem, recv_sem)
    me = ring.me
    rows_of = ring.rows_of

    ring.greet()
    for sub in range(SUBS):
        for r in range(RINGS):
            own = dy_ref.at[pl.ds(r * piece + sub * sub_rows, sub_rows), :]
            ring.message(r, 0, sub, sub, own).start()

    mine = pl.ds(pl.multiple_of(me * rows, rows), rows)
    bounce = [blk.at[pl.ds(i * rows, rows), :] for i in range(2)]
    for i, ref in enumerate((dy_ref, x_ref)):
        pltpu.make_async_copy(ref, bounce[i], wd_sem.at[i]).start()
    for i, ref in enumerate((dy_ref, x_ref)):
        pltpu.make_async_copy(ref, bounce[i], wd_sem.at[i]).wait()
        pltpu.make_async_copy(bounce[i], full_ref.at[i, mine, :], wd_sem.at[i]).start()
    for i in range(2):
        pltpu.make_async_copy(bounce[i], full_ref.at[i, mine, :], wd_sem.at[i]).wait()

    def serve(index):
        ring.serve(index, index, messages)

    units = FETCH + TILE_A * tiles_a + tiles_b
    first = (per_block - 1) * SUBS
    paced = messages - TAIL

    def serve_between(block, since, until):
        def served(unit):
            return first + (block * units + unit) * (paced - first) // (blocks * units)

        lax.fori_loop(served(since), served(until), lambda i, c: serve(i), None)

    def load_wd(j, slot):
        src = wd_ref.at[pl.ds(pl.multiple_of(j * tile_f, tile_f), tile_f), :]
        return pltpu.make_async_copy(src, wd_buf.at[slot], wd_sem.at[slot])

    def load_w2(j, slot):
        at = pl.ds(pl.multiple_of(j * tile_d, tile_d), tile_d)
        return [
            pltpu.make_async_copy(ref.at[at, :], w2_buf.at[slot, i], w2_sem.at[slot, i])
            for i, ref in enumerate((wg_ref, wu_ref))
        ]

    def pieces(block, body):
        def by_distance(i, carry):
            for r in range(RINGS):
                body(
                    rows_of(r, block * per_block + i),
                    pl.multiple_of(i * rows + r * piece, piece),
                )

        lax.fori_loop(0, per_block, by_distance, None)

    load_wd(0, 0).start()
    lax.fori_loop(0, first, lambda i, c: serve(i), None)

    def one_block(block, carry):
        for c in load_w2(0, 0):
            c.start()

        def fetch(there, here):
            pltpu.make_async_copy(full_ref.at[0, pl.ds(there, piece), :], blk.at[pl.ds(here, piece), :], blk_sem).start()
            for i, ref in enumerate((gate_ref, up_ref)):
                pltpu.make_async_copy(
                    ref.at[pl.ds(there, piece), :], gu_buf.at[i, pl.ds(here, piece), :], gu_sem.at[i]
                ).start()

        pieces(block, fetch)
        serve_between(block, 0, FETCH)
        pltpu.make_async_copy(full_ref.at[0, pl.ds(0, blk.shape[0]), :], blk, blk_sem).wait()
        for i, ref in enumerate((gate_ref, up_ref)):
            pltpu.make_async_copy(ref.at[pl.ds(0, blk.shape[0]), :], gu_buf.at[i], gu_sem.at[i]).wait()

        def tile_a_body(j, carry):
            slot = j % 2
            load_wd(j, slot).wait()

            @pl.when(j + 1 < tiles_a)
            def _():
                load_wd(j + 1, 1 - slot).start()

            dh_buf[...] = lax.dot_general(blk[...], wd_buf[slot], NT, preferred_element_type=F32)
            cols = pl.ds(pl.multiple_of(j * tile_f, tile_f), tile_f)
            chunk = 32

            def elementwise(i, c):
                at = pl.ds(pl.multiple_of(i * chunk, chunk), chunk)
                h, dgate, dup = act_grads(
                    gu_buf[0, at, cols].astype(F32), gu_buf[1, at, cols].astype(F32), dh_buf[at, :]
                )
                grads[0, at, cols] = dgate.astype(BF16)
                grads[1, at, cols] = dup.astype(BF16)
                grads[2, at, cols] = h.astype(BF16)

            lax.fori_loop(0, blk.shape[0] // chunk, elementwise, None, unroll=4)
            serve_between(block, FETCH + TILE_A * j, FETCH + TILE_A * (j + 1))

        lax.fori_loop(0, tiles_a, tile_a_body, None)

        def put_grads(there, here):
            for i, ref in enumerate((dg_ref, du_ref, hid_ref)):
                pltpu.make_async_copy(
                    grads.at[i, pl.ds(here, piece), :], ref.at[pl.ds(there, piece), :], grads_sem.at[i]
                ).start()

        pieces(block, put_grads)

        @pl.when(block + 1 < blocks)
        def _():
            load_wd(0, 0).start()

        def tile_b_body(j, carry):
            slot = j % 2
            for c in load_w2(j, slot):
                c.wait()

            @pl.when(j + 1 < tiles_b)
            def _():
                for c in load_w2(j + 1, 1 - slot):
                    c.start()

            blk[:, pl.ds(pl.multiple_of(j * tile_d, tile_d), tile_d)] = (
                lax.dot_general(grads[0], w2_buf[slot, 0], NT, preferred_element_type=F32)
                + lax.dot_general(grads[1], w2_buf[slot, 1], NT, preferred_element_type=F32)
            ).astype(BF16)

            @pl.when(j % GROUP == GROUP - 1)
            def _():
                width = GROUP * tile_d
                cols = pl.ds(pl.multiple_of(j // GROUP * width, width), width)

                def put(there, here):
                    pltpu.make_async_copy(
                        blk.at[pl.ds(here, piece), cols], dx_ref.at[pl.ds(there, piece), cols], o_sem
                    ).start()

                pieces(block, put)

            done = FETCH + TILE_A * tiles_a + j
            serve_between(block, done, done + 1)

        lax.fori_loop(0, tiles_b, tile_b_body, None)
        pltpu.make_async_copy(blk, dx_ref.at[pl.ds(0, blk.shape[0]), :], o_sem).wait()
        for i, ref in enumerate((dg_ref, du_ref, hid_ref)):
            pltpu.make_async_copy(grads.at[i], ref.at[pl.ds(0, blk.shape[0]), :], grads_sem.at[i]).wait()

    assert all(first + b * (paced - first) // blocks >= ((b + 1) * per_block - 1) * SUBS for b in range(blocks))
    lax.fori_loop(0, blocks, one_block, None)
    lax.fori_loop(paced, messages, lambda i, c: serve(i), None)
    ring.sent(messages)


def gather(mesh, x, dy, gate, up, w_gate, w_up, w_down, tile_f=256, tile_d=512, block=512):
    n = mesh.shape["tp"]
    rows, d_model = x.shape
    total, ff = gate.shape
    tile_f, tile_d, block = min(tile_f, ff), min(tile_d, d_model), min(block, total)
    hbm = pl.BlockSpec(memory_space=pl.ANY)
    kept = jax.ShapeDtypeStruct((total, ff), BF16)
    messages = (2 * (n - 1) - LATE) * SUBS
    return pl.pallas_call(
        functools.partial(gather_kernel, n, tile_f, tile_d),
        name="gather",
        out_shape=(
            jax.ShapeDtypeStruct((2, total, d_model), BF16),
            kept, kept, kept,
            jax.ShapeDtypeStruct((total, d_model), BF16),
        ),
        in_specs=[hbm] * 7,
        out_specs=(hbm,) * 5,
        scratch_shapes=[
            pltpu.VMEM((block, d_model), BF16),
            pltpu.VMEM((2, tile_f, d_model), BF16),
            pltpu.VMEM((2, 2, tile_d, ff), BF16),
            pltpu.VMEM((2, block, ff), BF16),
            pltpu.VMEM((block, tile_f), F32),
            pltpu.VMEM((3, block, ff), BF16),
            pltpu.SemaphoreType.DMA,
            pltpu.SemaphoreType.DMA((RINGS, messages)),
            pltpu.SemaphoreType.DMA,
            pltpu.SemaphoreType.DMA((2,)),
            pltpu.SemaphoreType.DMA((2, 2)),
            pltpu.SemaphoreType.DMA((2,)),
            pltpu.SemaphoreType.DMA((3,)),
            pltpu.SemaphoreType.DMA,
        ],
        compiler_params=pltpu.CompilerParams(collective_id=0, has_side_effects=True, vmem_limit_bytes=58 * 2**20),
        cost_estimate=pl.CostEstimate(
            flops=6 * total * d_model * ff, bytes_accessed=2 * 4 * 3 * ff * d_model, transcendentals=total * ff
        ),
    )(x, dy, gate, up, w_gate, w_up, w_down)


def late_kernel(
    n, tile_d,
    full_in_ref, hidden_ref,
    full_ref, dw_ref,
    hid, dy_buf, obuf,
    send_sem, recv_sem, hid_sem, dy_sem, o_sem,
):
    del full_in_ref
    total, d_model = full_ref.shape[1:]
    ff = hidden_ref.shape[1]
    tiles = d_model // tile_d
    ring = Ring(n, total // n, full_ref, send_sem, recv_sem)
    stop = 2 * ring.hops * SUBS
    messages = LATE * SUBS
    first = stop - messages

    ring.greet()
    for sub in range(SUBS):
        for r in range(RINGS):
            ring.message(r, first // SUBS, sub, sub).start()

    load = pltpu.make_async_copy(hidden_ref, hid, hid_sem)
    load.start()

    def load_dy(j, slot):
        at = pl.ds(pl.multiple_of(j * tile_d, tile_d), tile_d)
        return pltpu.make_async_copy(full_ref.at[0, :, at], dy_buf.at[slot], dy_sem.at[slot])

    def store(j, slot):
        at = pl.ds(pl.multiple_of(j * tile_d, tile_d), tile_d)
        return pltpu.make_async_copy(obuf.at[slot], dw_ref.at[:, at], o_sem.at[slot])

    load_dy(0, 0).start()
    load.wait()

    def tile(j, carry):
        slot = j % 2
        load_dy(j, slot).wait()

        @pl.when(j + 1 < tiles)
        def _():
            load_dy(j + 1, 1 - slot).start()

        @pl.when(j >= 2)
        def _():
            store(j - 2, slot).wait()

        obuf[slot] = lax.dot_general(hid[...], dy_buf[slot], TN, preferred_element_type=F32).astype(BF16)
        store(j, slot).start()
        lax.fori_loop(
            j * messages // tiles,
            (j + 1) * messages // tiles,
            lambda i, c: ring.serve(first + i, i, stop),
            None,
        )

    lax.fori_loop(0, tiles, tile, None)
    for j in (tiles - 2, tiles - 1):
        store(j, j % 2).wait()
    ring.sent(messages)


def finish(mesh, full, hidden, tile_d=512):
    n = mesh.shape["tp"]
    _, total, d_model = full.shape
    ff = hidden.shape[1]
    hbm = pl.BlockSpec(memory_space=pl.ANY)
    return pl.pallas_call(
        functools.partial(late_kernel, n, tile_d),
        name="finish",
        out_shape=(jax.ShapeDtypeStruct(full.shape, BF16), jax.ShapeDtypeStruct((ff, d_model), BF16)),
        in_specs=[hbm] * 2,
        out_specs=(hbm,) * 2,
        input_output_aliases={0: 0},
        scratch_shapes=[
            pltpu.VMEM((total, ff), BF16),
            pltpu.VMEM((2, total, tile_d), BF16),
            pltpu.VMEM((2, ff, tile_d), BF16),
            pltpu.SemaphoreType.DMA,
            pltpu.SemaphoreType.DMA((RINGS, LATE * SUBS)),
            pltpu.SemaphoreType.DMA,
            pltpu.SemaphoreType.DMA((2,)),
            pltpu.SemaphoreType.DMA((2,)),
        ],
        compiler_params=pltpu.CompilerParams(collective_id=1, has_side_effects=True, vmem_limit_bytes=60 * 2**20),
        cost_estimate=pl.CostEstimate(
            flops=2 * total * d_model * ff, bytes_accessed=2 * (total * ff + total * d_model + ff * d_model), transcendentals=0
        ),
    )(full, hidden)


def copy_kernel(src_ref, out_ref, buf, in_sem, out_sem):
    slots, rows, _ = buf.shape
    ahead = slots // 2
    chunks = src_ref.shape[0] // rows

    def chunk(ref, i):
        return ref.at[pl.ds(pl.multiple_of(i * rows, rows), rows), :]

    def load(i):
        return pltpu.make_async_copy(chunk(src_ref, i), buf.at[i % slots], in_sem.at[i % slots])

    def store(i):
        return pltpu.make_async_copy(buf.at[i % slots], chunk(out_ref, i), out_sem.at[i % slots])

    for i in range(ahead):
        load(i).start()

    def step(i, carry):
        load(i).wait()
        store(i).start()

        @pl.when(jnp.logical_and(i + ahead >= slots, i + ahead < chunks))
        def _():
            store(i + ahead - slots).wait()

        @pl.when(i + ahead < chunks)
        def _():
            load(i + ahead).start()

    lax.fori_loop(0, chunks, step, None)
    for i in range(chunks - slots, chunks):
        store(i).wait()


def copied(a, rows=64, slots=8):
    hbm = pl.BlockSpec(memory_space=pl.ANY)
    return pl.pallas_call(
        copy_kernel,
        name="copied",
        out_shape=jax.ShapeDtypeStruct(a.shape, a.dtype),
        in_specs=[hbm],
        out_specs=hbm,
        scratch_shapes=[
            pltpu.VMEM((slots, rows, a.shape[1]), a.dtype),
            pltpu.SemaphoreType.DMA((slots,)),
            pltpu.SemaphoreType.DMA((slots,)),
        ],
        compiler_params=pltpu.CompilerParams(vmem_limit_bytes=60 * 2**20),
        cost_estimate=pl.CostEstimate(flops=a.size, bytes_accessed=4 * a.size, transcendentals=0),
    )(a)


def solution(mesh):
    rows = P(("dp", "tp"), None)
    both = P("dp", "tp")
    cols = P(None, "tp")

    def body(x, dy, gate, up, w_gate, w_up, w_down):
        full, d_gate, d_up, hidden, dx = gather(mesh, x, dy, gate, up, w_gate, w_up, w_down)
        dx = lax.psum_scatter(dx, "tp", scatter_dimension=0, tiled=True)
        full, dw_down = finish(mesh, full, hidden)

        def dw(a, b):
            return lax.dot_general(a, b, TN, preferred_element_type=F32).astype(BF16)

        return dx, dw(full[1], d_gate), dw(full[1], d_up), copied(dw_down)

    return jax.shard_map(
        body,
        mesh=mesh,
        in_specs=(rows, rows, both, both, cols, cols, P("tp", None)),
        out_specs=(rows, both, both, rows),
        check_vma=False,
    )
```
